32 devices in a mesh: tm: 8 (over z, core), rows: 4 (over y, x).
Axes of the slice: x: 2, y: 2, z: 4, core: 2. Of those that a mesh axis runs over, the one named last changes fastest.
Arguments:
- frames_in: bfloat16 [16, 16, 120, 128], P('tm', 'rows'), may hold values from -25 to 25, as said below
- norm_gain: float32 [128], replicated, may hold values from 0.25 to 1.75
- norm_bias: float32 [128], replicated, may hold values from -0.5 to 0.5
- conv_weight: bfloat16 [3, 3, 3, 128, 128], replicated, may hold values from -0.109375 to 0.109375
- cotangent: bfloat16 [16, 16, 120, 128], P('tm', 'rows'), may hold values from -6 to 6
Outputs:
- output_frames: bfloat16 [16, 16, 120, 128], P('tm', 'rows')
- input_grad: bfloat16 [16, 16, 120, 128], P('tm', 'rows')
- weight_grad: float32 [128, 3456], P('rows')
- gain_grad: float32 [128], replicated
- bias_grad: float32 [128], replicated
The draws below stay inside these ranges and needn't reach their ends.
Inputs may be any that keep to these rules, and one draw needn't show every extreme that they name: Entries of frames_in lie within 25 in magnitude.
All inputs are finite; a program needn't handle non-finite values.
Results may differ from the reference program's by a relative error of at most 0.0042.
Values may be sent and summed in bfloat16 or wider, within the bound.
A program may use at most 64 MiB of HBM per device.

```python
import math
import jax
import jax.numpy as jnp
from jax import lax

C = 128
G = 32
W = 120
NT = 16
NH = 16


def draw_frames_in(key, part):
    keys_all = jax.random.split(key, 4)
    dims_all = (NT, NH, W, C)
    base_draw = jnp.clip(jax.random.normal(keys_all[0], dims_all, jnp.float32), -6.0, 6.0)
    time_pos = jnp.arange(NT, dtype=jnp.float32) / max(NT - 1, 1)
    height_pos = jnp.arange(NH, dtype=jnp.float32) / max(NH - 1, 1)
    frame_scale = 3.0 ** time_pos * jnp.exp(jax.random.uniform(keys_all[1], (NT,), jnp.float32, -0.35, 0.35))
    row_scale = 3.0 ** height_pos * jnp.exp(jax.random.uniform(keys_all[2], (NH,), jnp.float32, -0.35, 0.35))
    chan_scale = jnp.exp(jax.random.uniform(keys_all[3], (C,), jnp.float32, -0.7, 0.7))
    scaled = 0.1 * base_draw * frame_scale[:, None, None, None] * row_scale[None, :, None, None] * chan_scale
    return scaled.astype(jnp.bfloat16)


def level_of(own_key, extent, cuts, low, high):
    def one(position, blocks):
        heights = jax.random.uniform(jax.random.fold_in(jax.random.fold_in(own_key, 6), position), (blocks,), jnp.float32, low / len(cuts), high / len(cuts))
        return jnp.repeat(jnp.exp(heights), extent[position] // blocks).reshape((-1,) + (1,) * (len(extent) - position - 1))

    level = one(*cuts[0])
    for cut in cuts[1:]:
        level = level * one(*cut)
    return level


def bell_draw(rng, extent, deviation, bound, cuts=(), held_as=jnp.bfloat16):
    drawn = jax.random.normal(rng, extent, jnp.float32) * deviation
    if len(cuts) > 0:
        drawn = level_of(rng, extent, cuts, -0.22, 0.18) * drawn
    return jnp.clip(drawn, min=-bound, max=bound).astype(held_as)


def setup_inputs(seed: int = 0) -> dict:
    seeds = jax.random.split(jax.random.key(seed), 6)
    return {
        "frames_in": draw_frames_in(jax.random.fold_in(seeds[5], 71), 0),
        "norm_gain": jnp.clip(1.0 + 0.15 * jax.random.normal(seeds[1], (C,), jnp.float32), 0.25, 1.75),
        "norm_bias": jnp.clip(jax.random.uniform(seeds[2], (C,), jnp.float32, -0.5, 0.5), -0.5, 0.5),
        "conv_weight": bell_draw(seeds[3], (3, 3, 3, C, C), (27 * C) ** -0.5, 0.109375),
        "cotangent": bell_draw(seeds[4], (NT, NH, W, C), 1.0, 6.0, ((0, 8), (1, 4))),
    }


EPSILON = 1e-06

def group_expand(per_channel):
    return jnp.repeat(per_channel.reshape(G, C // G).sum(axis=1), C // G)

def reference(frames_in, norm_gain, norm_bias, conv_weight, cotangent):
    total_cells = NT * NH * W * (C // G)
    values = frames_in.astype(jnp.float32)
    channel_sum = lax.optimization_barrier(jnp.sum(values, axis=(0, 1, 2)))
    channel_sq = lax.optimization_barrier(jnp.sum(values * values, axis=(0, 1, 2)))
    group_mean = group_expand(channel_sum) / total_cells
    variance = group_expand(channel_sq) / total_cells - group_mean * group_mean
    inverse_std = lax.rsqrt(variance + EPSILON)
    normed = (values - group_mean) * inverse_std
    preact = normed * norm_gain + norm_bias
    activated = jax.nn.silu(preact).astype(jnp.bfloat16)
    padded = jnp.pad(activated, ((2, 0), (1, 1), (1, 1), (0, 0)))
    grad_padded = jnp.pad(cotangent, ((0, 2), (1, 1), (1, 1), (0, 0)))
    grad_flat = cotangent.reshape(-1, C)
    conv_sum = jnp.zeros((NT * NH * W, C), jnp.float32)
    grad_act = jnp.zeros((NT * NH * W, C), jnp.float32)
    pieces = []
    for time_off in range(3):
        for row_off in range(3):
            for col_off in range(3):
                window = padded[time_off:time_off + NT, row_off:row_off + NH, col_off:col_off + W].reshape(-1, C)
                conv_sum = conv_sum + jnp.dot(window, conv_weight[time_off, row_off, col_off], preferred_element_type=jnp.float32)
                pieces.append(lax.dot_general(grad_flat, window, (((0,), (0,)), ((), ())), preferred_element_type=jnp.float32))
                grad_window = grad_padded[time_off:time_off + NT, row_off:row_off + NH, col_off:col_off + W].reshape(-1, C)
                flipped = conv_weight[2 - time_off, 2 - row_off, 2 - col_off].T
                grad_act = grad_act + jnp.dot(grad_window, flipped, preferred_element_type=jnp.float32)
    output_frames = (values + conv_sum.reshape(values.shape)).astype(jnp.bfloat16)
    weight_grad = jnp.concatenate(pieces, axis=1) * (1.0 / math.sqrt(NT * NH * W))
    sigmoid_v = jax.nn.sigmoid(preact)
    grad_pre = grad_act.reshape(values.shape) * sigmoid_v * (1.0 + preact * (1.0 - sigmoid_v))
    gain_grad = lax.optimization_barrier(jnp.sum(grad_pre * normed, axis=(0, 1, 2)))
    bias_grad = lax.optimization_barrier(jnp.sum(grad_pre, axis=(0, 1, 2)))
    mean_dn = group_expand(norm_gain * bias_grad) / total_cells
    mean_dnn = group_expand(norm_gain * gain_grad) / total_cells
    input_grad = inverse_std * (grad_pre * norm_gain - mean_dn - normed * mean_dnn) + cotangent.astype(jnp.float32)
    return (output_frames, input_grad.astype(jnp.bfloat16), weight_grad, gain_grad, bias_grad)
```

```python
import functools
import math

import jax
import jax.numpy as jnp
from jax import lax
from jax.experimental import pallas as pl
from jax.experimental.pallas import tpu as pltpu
from jax.sharding import PartitionSpec as P

G = 32
EPSILON = 1e-06
MESH = pl.DeviceIdType.MESH
F32, BF16 = jnp.float32, jnp.bfloat16
LANES = 128


def sigmoid(v):
    return 1.0 / (1.0 + jnp.exp(-v))


def group_total(x, width):
    lanes = x.shape[-1]
    lane = lax.broadcasted_iota(jnp.int32, x.shape, len(x.shape) - 1)
    shift = 1
    while shift < width:
        up = pltpu.roll(x, lanes - shift, axis=len(x.shape) - 1)
        down = pltpu.roll(x, shift, axis=len(x.shape) - 1)
        x = x + jnp.where((lane & shift) == 0, up, down)
        shift *= 2
    return x


def kernel(
    dims,
    x_ref, gain_ref, bias_ref, w_ref, g_ref,
    out_ref, ingrad_ref, wgrad_ref, ggain_ref, gbias_ref,
    fext, cext, x3, g3, gt, gact, gpre,
    wf, wb, arecv, bsend, brecv, csend, crecv, fin,
    st_r, st_t, gb_r, gb_t,
    halo_send, halo_recv, st_send, st_recv, gb_send, gb_recv,
    a_send, a_recv, b_send, b_recv, c_send, c_recv, d_send, d_recv,
):
    n_tm, n_rows, o_per, piece = dims
    n_z = n_tm // 2
    half = n_z * piece
    frames, band, cols, channels = x_ref.shape
    wide = x3.shape[2]
    width = channels // G
    pixels = frames * n_tm * band * n_rows * cols
    cells = pixels * width
    tm, r = lax.axis_index("tm"), lax.axis_index("rows")
    core, z = lax.rem(tm, 2), lax.div(tm, 2)

    fext[0:2] = jnp.zeros((2, band + 2, cols, channels), BF16)
    fext[2:4, 0:1] = jnp.zeros((2, 1, cols, channels), BF16)
    fext[2:4, band + 1 : band + 2] = jnp.zeros((2, 1, cols, channels), BF16)
    cext[2:4] = jnp.zeros((2, band + 2, cols, channels), BF16)
    cext[0:2, 0:1] = jnp.zeros((2, 1, cols, channels), BF16)
    cext[0:2, band + 1 : band + 2] = jnp.zeros((2, 1, cols, channels), BF16)

    def there(dt, dr):
        ok = None
        for ind, delta, n in ((tm, dt, n_tm), (r, dr, n_rows)):
            if delta:
                this = (ind + delta >= 0) & (ind + delta < n)
                ok = this if ok is None else ok & this
        return ok

    barrier = pltpu.get_barrier_semaphore()
    for d in range(1, n_rows):
        pl.semaphore_signal(barrier, inc=1, device_id=(tm, lax.rem(r + d, n_rows)), device_id_type=MESH)
    for d in range(1, n_tm):
        pl.semaphore_signal(barrier, inc=1, device_id=(lax.rem(tm + d, n_tm), r), device_id_type=MESH)
    greeted = n_rows - 1 + n_tm - 1
    for dt in (-1, 1):
        for dr in (-1, 1):
            ok = there(dt, dr)
            greeted = greeted + jnp.where(ok, 1, 0)

            @pl.when(ok)
            def _():
                pl.semaphore_signal(barrier, inc=1, device_id=(tm + dt, r + dr), device_id_type=MESH)

    def stat_step(p, carry):
        s, q = carry
        v = x_ref[lax.div(p, band), lax.rem(p, band)].astype(F32)
        v = v.reshape(cols // 8, 8, channels)
        return s + jnp.sum(v, axis=0), q + jnp.sum(v * v, axis=0)

    zero8 = jnp.zeros((8, channels), F32)
    s8, q8 = lax.fori_loop(0, frames * band, stat_step, (zero8, zero8))
    row8 = lax.broadcasted_iota(jnp.int32, (8, channels), 0)

    def two_rows(first, second):
        a = jnp.sum(first, axis=0, keepdims=True)
        b = jnp.sum(second, axis=0, keepdims=True)
        return jnp.where(row8 == 0, a, jnp.where(row8 == 1, b, 0.0))

    st_r[r] = two_rows(s8, q8)
    pl.semaphore_wait(barrier, greeted)

    def remote(src, dst, ssem, rsem, dev):
        return pltpu.make_async_remote_copy(
            src_ref=src, dst_ref=dst, send_sem=ssem, recv_sem=rsem, device_id=dev, device_id_type=MESH
        )

    def rows_copies(buf, ssem, rsem, incoming):
        made = []
        for d in range(1, n_rows):
            slot = lax.rem(r + n_rows - d, n_rows) if incoming else r
            made.append(remote(buf.at[slot], buf.at[slot], ssem.at[d - 1], rsem.at[d - 1], (tm, lax.rem(r + d, n_rows))))
        return made

    def tm_copies(buf, ssem, rsem, incoming):
        made = []
        for d in range(1, n_tm):
            slot = lax.rem(tm + n_tm - d, n_tm) if incoming else tm
            k = n_rows - 2 + d
            made.append(remote(buf.at[slot], buf.at[slot], ssem.at[k], rsem.at[k], (lax.rem(tm + d, n_tm), r)))
        return made

    def start_all(copies):
        for copy in copies:
            copy.start()

    def wait_recv(copies):
        for copy in copies:
            copy.wait_recv()

    def wait_send(copies):
        for copy in copies:
            copy.wait_send()

    def slot_sum(buf, n):
        total = buf[0]
        for j in range(1, n):
            total = total + buf[j]
        return total

    start_all(rows_copies(st_r, st_send, st_recv, False))

    last = slice(band - 1, band)
    first = slice(0, 1)
    body = slice(1, band + 1)
    top, bottom = slice(0, 1), slice(band + 1, band + 2)
    every = slice(None)
    halos = [
        (g_ref, cext, (0, 1), last, slice(0, 2), top),
        (g_ref, cext, (0, -1), first, slice(0, 2), bottom),
        (g_ref, cext, (-1, 1), last, slice(2, 4), top),
        (g_ref, cext, (-1, -1), first, slice(2, 4), bottom),
        (g_ref, cext, (-1, 0), every, slice(2, 4), body),
        (x_ref, fext, (0, 1), last, slice(2, 4), top),
        (x_ref, fext, (0, -1), first, slice(2, 4), bottom),
        (x_ref, fext, (1, 1), last, slice(0, 2), top),
        (x_ref, fext, (1, -1), first, slice(0, 2), bottom),
        (x_ref, fext, (1, 0), every, slice(0, 2), body),
    ]

    def halo_copy(k):
        src, dst, (dt, dr), rows_from, frames_to, rows_to = halos[k]
        return remote(
            src.at[:, rows_from], dst.at[frames_to, rows_to], halo_send.at[k], halo_recv.at[k], (tm + dt, r + dr)
        )

    for k in range(len(halos)):
        dt, dr = halos[k][2]

        @pl.when(there(dt, dr))
        def _(k=k):
            halo_copy(k).start()

    def halo_wait_recv(ks):
        for k in ks:
            dt, dr = halos[k][2]

            @pl.when(there(-dt, -dr))
            def _(k=k):
                halo_copy(k).wait_recv()

    pad_rows = jnp.zeros((wide - cols, channels), F32)

    def three_shifts(dst, f, h, v):
        v = jnp.concatenate([v, pad_rows], axis=0)
        dst[f, h, :, 0:channels] = pltpu.roll(v, 1, axis=0).astype(BF16)
        dst[f, h, :, channels : 2 * channels] = v.astype(BF16)
        dst[f, h, :, 2 * channels : 3 * channels] = pltpu.roll(v, wide - 1, axis=0).astype(BF16)

    def own_cot(p, carry):
        f, h = lax.div(p, band), lax.rem(p, band)
        three_shifts(g3, f, h + 1, g_ref[f, h].astype(F32))
        return carry

    lax.fori_loop(0, frames * band, own_cot, 0)
    own = g3[0:frames, 1 : band + 1, :, channels : 2 * channels].reshape(frames * band * wide, channels)
    gt[...] = own.T

    wait_recv(rows_copies(st_r, st_send, st_recv, True))
    st_t[tm] = slot_sum(st_r, n_rows)
    start_all(tm_copies(st_t, st_send, st_recv, False))

    halo_wait_recv(range(0, 5))

    def edge_cot(p, carry):
        f, h = lax.div(p, 2), lax.rem(p, 2) * (band + 1)
        three_shifts(g3, f, h, cext[f, h].astype(F32))
        return carry

    lax.fori_loop(0, 2 * frames, edge_cot, 0)

    def next_cot(p, carry):
        f, h = lax.div(p, band + 2) + frames, lax.rem(p, band + 2)
        three_shifts(g3, f, h, cext[f, h].astype(F32))
        return carry

    lax.fori_loop(0, frames * (band + 2), next_cot, 0)

    plane = band * wide
    for t in range(frames):
        acc = jnp.zeros((plane, channels), F32)
        for a in range(3):
            for b in range(3):
                rhs = jnp.concatenate([w_ref[2 - a, 2 - b, 2 - c] for c in range(3)], axis=1)
                acc = acc + lax.dot_general(
                    g3[t + a, b : b + band].reshape(plane, 3 * channels),
                    rhs,
                    (((1,), (1,)), ((), ())),
                    preferred_element_type=F32,
                )
        gact[t] = acc.reshape(band, wide, channels)

    wait_recv(tm_copies(st_t, st_send, st_recv, True))
    stats = group_total(slot_sum(st_t, n_tm), width) / cells
    mean = stats[0:1]
    inverse_std = lax.rsqrt(stats[1:2] - mean * mean + EPSILON)
    gain, bias = gain_ref[...], bias_ref[...]

    halo_wait_recv(range(5, 10))

    def act_rows(f, h, v, keep):
        preact = (v.astype(F32) - mean) * inverse_std * gain + bias
        three_shifts(x3, f, h, preact * sigmoid(preact) * keep)

    def own_act(p, carry):
        f, h = lax.div(p, band), lax.rem(p, band)
        act_rows(f + 2, h + 1, x_ref[f, h], 1.0)
        return carry

    lax.fori_loop(0, frames * band, own_act, 0)

    def keep_of(f, h):
        dead = ((f < 2) & (tm == 0)) | ((h == 0) & (r == 0)) | ((h == band + 1) & (r == n_rows - 1))
        return jnp.where(dead, 0.0, 1.0)

    def edge_act(p, carry):
        f, h = lax.div(p, 2) + 2, lax.rem(p, 2) * (band + 1)
        act_rows(f, h, fext[f, h], keep_of(f, h))
        return carry

    lax.fori_loop(0, 2 * frames, edge_act, 0)

    def cached_act(p, carry):
        f, h = lax.div(p, band + 2), lax.rem(p, band + 2)
        act_rows(f, h, fext[f, h], keep_of(f, h))
        return carry

    lax.fori_loop(0, 2 * (band + 2), cached_act, 0)

    rows_used = 27 * o_per
    if rows_used < 2 * half:
        wf[:, rows_used:] = jnp.zeros((n_rows, 2 * half - rows_used, channels), F32)
        wb[:, rows_used:] = jnp.zeros((n_rows, 2 * half - rows_used, channels), BF16)
    for a in range(3):
        for b in range(3):
            res = jnp.dot(
                gt[...],
                x3[a : a + frames, b : b + band].reshape(frames * plane, 3 * channels),
                preferred_element_type=F32,
            )
            for c in range(3):
                at = (9 * a + 3 * b + c) * o_per
                tile = res[:, c * channels : (c + 1) * channels].reshape(n_rows, o_per, channels)
                wf[:, at : at + o_per] = tile
                wb[:, at : at + o_per] = tile.astype(BF16)

    mine = pl.ds(pl.multiple_of(core * half, 16), half)
    other = pl.ds(pl.multiple_of((1 - core) * half, 16), half)
    stage_a = remote(wb.at[:, other], arecv, a_send, a_recv, (tm + 1 - 2 * core, r))
    stage_a.start()

    def forward(t):
        acc = jnp.zeros((plane, channels), F32)
        for a in range(3):
            for b in range(3):
                acc = acc + jnp.dot(
                    x3[t + a, b : b + band].reshape(plane, 3 * channels),
                    w_ref[a, b].reshape(3 * channels, channels),
                    preferred_element_type=F32,
                )
        acc = acc.reshape(band, wide, channels)[:, :cols]
        out_ref[t] = (x_ref[t].astype(F32) + acc).astype(BF16)

    forward(0)

    stage_a.wait_recv()
    summed = wf[:, mine] + arecv[...].astype(F32)
    wf[:, mine] = summed
    bsend[...] = summed.astype(BF16)
    stage_b = []
    for d in range(1, n_rows):
        to = lax.rem(r + d, n_rows)
        stage_b.append(remote(bsend.at[to], brecv.at[d - 1], b_send.at[d - 1], b_recv.at[d - 1], (tm, to)))
    start_all(stage_b)

    def pre_step(p, carry):
        s, q = carry
        t, h = lax.div(p, band), lax.rem(p, band)
        normed = (x_ref[t, h].astype(F32) - mean) * inverse_std
        preact = normed * gain + bias
        sig = sigmoid(preact)
        gp = gact[t, h, 0:cols] * sig * (1.0 + preact * (1.0 - sig))
        gpre[t, h] = gp
        prod = (gp * normed).reshape(cols // 8, 8, channels)
        return s + jnp.sum(prod, axis=0), q + jnp.sum(gp.reshape(cols // 8, 8, channels), axis=0)

    s8, q8 = lax.fori_loop(0, frames * band, pre_step, (zero8, zero8))
    gb_r[r] = two_rows(s8, q8)
    start_all(rows_copies(gb_r, gb_send, gb_recv, False))

    for t in range(1, frames):
        forward(t)

    wait_recv(rows_copies(gb_r, gb_send, gb_recv, True))
    gb_t[tm] = slot_sum(gb_r, n_rows)
    start_all(tm_copies(gb_t, gb_send, gb_recv, False))

    wait_recv(stage_b)
    total = wf[r, mine]
    for d in range(1, n_rows):
        total = total + brecv[d - 1].astype(F32)
    wf[r, mine] = total
    csend[...] = total.astype(BF16)
    stage_c = []
    for d in range(1, n_z):
        to = lax.rem(z + d, n_z)
        chunk = pl.ds(pl.multiple_of(to * piece, 16), piece)
        stage_c.append(
            remote(csend.at[chunk], crecv.at[d - 1], c_send.at[d - 1], c_recv.at[d - 1], (2 * to + core, r))
        )
    start_all(stage_c)

    wait_recv(tm_copies(gb_t, gb_send, gb_recv, True))
    both = slot_sum(gb_t, n_tm)
    ggain_ref[...] = both[0:1]
    gbias_ref[...] = both[1:2]
    means = group_total(both * gain, width) / cells
    mean_dnn, mean_dn = means[0:1], means[1:2]

    wait_recv(stage_c)
    total = wf[r, pl.ds(pl.multiple_of(core * half + z * piece, 16), piece)]
    for d in range(1, n_z):
        total = total + crecv[d - 1].astype(F32)
    spot = pl.ds(pl.multiple_of(core * half + z * piece, 16), piece)
    fin[spot] = (total * (1.0 / math.sqrt(pixels))).astype(BF16)
    stage_d, stage_d_in = [], []
    for d in range(1, n_tm):
        to, frm = lax.rem(tm + d, n_tm), lax.rem(tm + n_tm - d, n_tm)
        theirs = pl.ds(pl.multiple_of(lax.rem(frm, 2) * half + lax.div(frm, 2) * piece, 16), piece)
        stage_d.append(remote(fin.at[spot], fin.at[spot], d_send.at[d - 1], d_recv.at[d - 1], (to, r)))
        stage_d_in.append(remote(fin.at[theirs], fin.at[theirs], d_send.at[d - 1], d_recv.at[d - 1], (to, r)))
    start_all(stage_d)

    def final_step(p, carry):
        t, h = lax.div(p, band), lax.rem(p, band)
        normed = (x_ref[t, h].astype(F32) - mean) * inverse_std
        grad = inverse_std * (gpre[t, h] * gain - mean_dn - normed * mean_dnn) + g_ref[t, h].astype(F32)
        ingrad_ref[t, h] = grad.astype(BF16)
        return carry

    lax.fori_loop(0, frames * band, final_step, 0)

    wait_recv(stage_d_in)
    for tap in range(27):
        wgrad_ref[:, tap * channels : (tap + 1) * channels] = fin[tap * o_per : (tap + 1) * o_per].astype(F32)

    for k in range(len(halos)):
        dt, dr = halos[k][2]

        @pl.when(there(dt, dr))
        def _(k=k):
            halo_copy(k).wait_send()

    wait_send(rows_copies(st_r, st_send, st_recv, False))
    wait_send(tm_copies(st_t, st_send, st_recv, False))
    wait_send(rows_copies(gb_r, gb_send, gb_recv, False))
    wait_send(tm_copies(gb_t, gb_send, gb_recv, False))
    stage_a.wait_send()
    wait_send(stage_b)
    wait_send(stage_c)
    wait_send(stage_d)


def per_device(frames_in, norm_gain, norm_bias, conv_weight, cotangent):
    frames, band, cols, channels = frames_in.shape
    n_tm, n_rows = lax.axis_size("tm"), lax.axis_size("rows")
    wide = -(-(cols + 1) // 16) * 16
    o_per = channels // n_rows
    n_z = n_tm // 2
    piece = -(-27 * o_per // (n_tm * 16)) * 16
    half = n_z * piece
    small = n_rows - 1 + n_tm - 1
    dma = pltpu.SemaphoreType.DMA
    vmem = pl.BlockSpec(memory_space=pltpu.VMEM)
    outs = pl.pallas_call(
        functools.partial(kernel, (n_tm, n_rows, o_per, piece)),
        out_shape=(
            jax.ShapeDtypeStruct(frames_in.shape, BF16),
            jax.ShapeDtypeStruct(frames_in.shape, BF16),
            jax.ShapeDtypeStruct((o_per, 27 * channels), F32),
            jax.ShapeDtypeStruct((1, channels), F32),
            jax.ShapeDtypeStruct((1, channels), F32),
        ),
        in_specs=[vmem] * 5,
        out_specs=(vmem,) * 5,
        scratch_shapes=[
            pltpu.VMEM((frames + 2, band + 2, cols, channels), BF16),
            pltpu.VMEM((frames + 2, band + 2, cols, channels), BF16),
            pltpu.VMEM((frames + 2, band + 2, wide, 3 * channels), BF16),
            pltpu.VMEM((frames + 2, band + 2, wide, 3 * channels), BF16),
            pltpu.VMEM((channels, frames * band * wide), BF16),
            pltpu.VMEM((frames, band, wide, channels), F32),
            pltpu.VMEM((frames, band, cols, channels), F32),
            pltpu.VMEM((n_rows, 2 * half, channels), F32),
            pltpu.VMEM((n_rows, 2 * half, channels), BF16),
            pltpu.VMEM((n_rows, half, channels), BF16),
            pltpu.VMEM((n_rows, half, channels), BF16),
            pltpu.VMEM((n_rows - 1, half, channels), BF16),
            pltpu.VMEM((half, channels), BF16),
            pltpu.VMEM((n_z - 1, piece, channels), BF16),
            pltpu.VMEM((2 * half, channels), BF16),
            pltpu.VMEM((n_rows, 8, channels), F32),
            pltpu.VMEM((n_tm, 8, channels), F32),
            pltpu.VMEM((n_rows, 8, channels), F32),
            pltpu.VMEM((n_tm, 8, channels), F32),
            dma((10,)), dma((10,)),
            dma((small,)), dma((small,)),
            dma((small,)), dma((small,)),
            dma, dma,
            dma((n_rows - 1,)), dma((n_rows - 1,)),
            dma((n_z - 1,)), dma((n_z - 1,)),
            dma((n_tm - 1,)), dma((n_tm - 1,)),
        ],
        compiler_params=pltpu.CompilerParams(
            collective_id=0, has_side_effects=True, vmem_limit_bytes=56 * 1024 * 1024
        ),
    )(frames_in, norm_gain.reshape(1, channels), norm_bias.reshape(1, channels), conv_weight, cotangent)
    return outs[0], outs[1], outs[2], outs[3].reshape(channels), outs[4].reshape(channels)


def solution(mesh):
    placed = (P("tm", "rows", None, None), P(), P(), P(), P("tm", "rows", None, None))
    return jax.shard_map(
        per_device,
        mesh=mesh,
        in_specs=placed,
        out_specs=(
            P("tm", "rows", None, None),
            P("tm", "rows", None, None),
            P("rows", None),
            P(),
            P(),
        ),
        check_vma=False,
    )
```
